128 devices in a mesh: row: 16 (over y, x_hi, core), col: 8 (over x_lo, z).
Axes of the slice: x: 4 (x_hi: 2, x_lo: 2; x = x_hi * 2 + x_lo), y: 4, z: 4, core: 2. Of those that a mesh axis runs over, the one named last changes fastest.
Arguments:
- matrix: float32 [8, 16, 128, 16, 8, 128], P(None, 'row', None, None, 'col'), may hold values from -6 to 6
- reflectors: float32 [16, 8, 128, 512], P(None, 'col'), as said below
Outputs:
- updated: float32 [8, 16, 128, 16, 8, 128], P(None, 'row', None, None, 'col')
The draws below stay inside these ranges and needn't reach their ends.
Inputs may be any that keep to these rules, and one draw needn't show every extreme that they name: Read as a 16384 x 512 matrix, the columns of reflectors are orthonormal.
All inputs are finite; a program needn't handle non-finite values.
Results may differ from the reference program's by a relative error of at most 0.0001.
Values sent between devices are 32-bit elements; how exact they have to be, the bound alone decides.
A program may use at most 128 MiB of HBM per device.

```python
import jax
import jax.numpy as jnp
from jax import lax

ORDER = 16384
TILE = 128
PANEL = 256
PANELS = 2
RT = 8
CT = 16
N_ROW = 16
N_COL = 8


def draw_reflectors(key, part):
    first_key = jax.random.fold_in(key, 11)
    source = jax.random.normal(first_key, (ORDER, PANEL * PANELS), jnp.float32)
    orthonormal, _ = jnp.linalg.qr(source)
    return orthonormal.reshape(CT, ORDER // (CT * TILE), TILE, PANEL * PANELS).astype(jnp.float32)


def level_of(own_key, dims, pieces, low, largest):
    def one(dim, shards_of):
        heights = jax.random.uniform(jax.random.fold_in(jax.random.fold_in(own_key, 6), dim), (shards_of,), jnp.float32, low / len(pieces), largest / len(pieces))
        return jnp.repeat(jnp.exp(heights), dims[dim] // shards_of).reshape((-1,) + (1,) * (len(dims) - dim - 1))

    factor_of = one(*pieces[0])
    for cut in pieces[1:]:
        factor_of = factor_of * one(*cut)
    return factor_of


def bell_draw(stream_key, shape, width, most, pieces=(), dtype=jnp.bfloat16):
    result = jax.random.normal(stream_key, shape, jnp.float32) * width
    if len(pieces) > 0:
        result = level_of(stream_key, shape, pieces, -0.22, 0.18) * result
    return jnp.clip(result, min=-most, max=most).astype(dtype)


def setup_inputs(seed: int = 0) -> dict:
    key_list = jax.random.split(jax.random.key(seed), 3)
    matrix = bell_draw(key_list[0], (RT, N_ROW, TILE, CT, N_COL, TILE), 1.0, 6.0, ((1, 16), (4, 8)), jnp.float32)
    reflectors = draw_reflectors(jax.random.fold_in(key_list[2], 71), 0)
    return dict(matrix=matrix, reflectors=reflectors)


def reference(matrix, reflectors):
    stored = matrix.reshape(ORDER, ORDER)
    current = jnp.tril(stored) + jnp.tril(stored, -1).T
    basis = reflectors.reshape(ORDER, PANEL * PANELS)
    for panel in range(PANELS):
        vectors = basis[:, panel * PANEL:(panel + 1) * PANEL]
        product = jnp.dot(current.astype(jnp.float32), vectors.astype(jnp.float32), precision=lax.Precision.HIGHEST, preferred_element_type=jnp.float32)
        projection = jnp.dot(vectors.T.astype(jnp.float32), product.astype(jnp.float32), precision=lax.Precision.HIGHEST, preferred_element_type=jnp.float32)
        product = product - 0.5 * jnp.dot(vectors.astype(jnp.float32), projection.astype(jnp.float32), precision=lax.Precision.HIGHEST, preferred_element_type=jnp.float32)
        left_side = jnp.concatenate([vectors, product], axis=1)
        right_side = jnp.concatenate([product, vectors], axis=1)
        current = current - jnp.dot(left_side.astype(jnp.float32), right_side.T.astype(jnp.float32), precision=lax.Precision.HIGHEST, preferred_element_type=jnp.float32)
    return jnp.tril(current).reshape(matrix.shape)
```

```python
import jax
import jax.numpy as jnp
from jax import lax
from jax.experimental import pallas as pl
from jax.experimental.pallas import tpu as pltpu
from jax.sharding import PartitionSpec as P

MESH = pl.DeviceIdType.MESH
F32 = jnp.float32
BF16 = jnp.bfloat16
NC = 4
PLAN = (
    ("prep", (2, 0, 3)), ("dc", (3,)), ("v1", (0,)), ("dc", (2,)), ("v1", (1,)), ("prep", (1,)), ("v1", (2,)),
    ("v2", (0,)), ("dc", (1, 0)), ("d1", (3,)), ("v2", (1,)), ("v1", (3,)), ("d1", (0,)), ("v3", (0, 1)),
    ("v2", (2,)), ("vt", (0,)), ("d1", (1,)), ("v2", (3,)), ("vt", (1,)), ("v3", (2,)), ("t2", (0,)), ("v3", (3,)),
    ("t2", (1,)), ("dx", (0,)), ("vt", (2,)), ("d1", (2,)), ("dx", (3, 1)), ("t3", (1, 0)), ("vt", (3,)),
    ("t2", (2,)), ("t4", (1,)), ("d2", (1,)), ("t4", (0,)), ("d2", (0,)), ("dx", (2,)), ("t3", (2,)), ("d3", (1,)),
    ("t5", (1,)), ("t2", (3,)), ("d3", (0,)), ("rz", (1,)), ("t4", (2,)), ("d2", (2,)), ("t5", (0,)), ("t3", (3,)),
    ("cx", (1,)), ("t5", (2,)), ("rz", (0,)), ("d2", (3,)), ("d3", (2,)), ("t4", (3,)), ("a2", (1,)), ("rz", (2,)),
    ("cx", (0,)), ("d3", (3,)), ("t5", (3,)), ("cx", (2,)), ("a3", (1,)), ("rz", (3,)), ("a2", (0,)), ("cx", (3,)),
    ("a2", (2,)), ("a3", (0,)), ("a2", (3,)), ("a3", (2,)), ("a4", (0, 1)), ("a3", (3,)), ("a4", (2,)), ("a5", (0,)),
    ("a4", (3,)), ("a5", (2, 1, 3)),
)
RANK = 512
W = RANK // NC
Q = W // 4
UW = W + Q

RINGS = ("V", "A", "B", "D", "T")
OPS = [a + b for a in RINGS for b in ("1", "2p", "2m", "3p", "3m", "4", "5p", "5m")]
OPS += ["V0", "CD", "CT"] + ["R1", "R2", "R3", "R4"]
OP = {name: n for n, name in enumerate(OPS)}


def split(x):
    hi = x.astype(BF16)
    return hi, (x - hi.astype(F32)).astype(BF16)


def dot(a, b):
    return jnp.dot(a, b, preferred_element_type=F32)


def dot_nt(a, b):
    return lax.dot_general(a, b, (((1,), (1,)), ((), ())), preferred_element_type=F32)


def block(i, j):
    return i * (i + 1) // 2 + j


def xor(a, b):
    return a + b - 2 * a * b


def exchange(
    mat, refl, out,
    sbuf, sh, sl, vc, vcs, vr, vrs, vrt, dbuf, dh, dl, dr, d2r,
    ubuf, t1r, t2r, t3r, crd, crt, rx, gbuf, wr, mm, wcts, wrs, zero,
    ssem, rsem, msem, vsem, osem,
):
    r, c = lax.axis_index("row"), lax.axis_index("col")
    div, rem = lax.div, lax.rem
    core, y = rem(r, 2), div(r, 4)
    xh = rem(div(r, 2), 2)
    z, xl = rem(c, 4), div(c, 4)
    half, low = div(r, 8), rem(r, 8)
    alone = low == c
    y0, z1, z0 = rem(y, 2), div(z, 2), rem(z, 2)
    yp, ym, y2 = rem(y + 1, 4), rem(y + 3, 4), rem(y + 2, 4)
    zp, zm, z2 = rem(z + 1, 4), rem(z + 3, 4), rem(z + 2, 4)
    to_core = {"row": r + 1 - 2 * core}
    to_xh = {"row": r + 2 - 4 * xh}
    to_yp, to_ym = {"row": yp * 4 + rem(r, 4)}, {"row": ym * 4 + rem(r, 4)}
    to_xl = {"col": c + 4 - 8 * xl}
    to_zp, to_zm = {"col": xl * 4 + zp}, {"col": xl * 4 + zm}
    flip = xor(z1, xl)
    to_t = {"row": half * 8 + 4 * xor(xor(z1, xh), y0) + 2 * xor(xor(xl, y0), xh) + z0, "col": low}
    dxl, dz1 = xor(xh, flip), xor(y0, flip)
    to_d = {"row": half * 8 + c, "col": dxl * 4 + dz1 * 2 + core}
    dz = dz1 * 2 + core
    own = 2 * (4 * xor(xh, z1) + 2 * dz1 + core) + half

    def row_slot(k):
        return k % 4, 1 - y0 if k // 4 else y0

    def col_slot(m):
        k, h = m // 2, m % 2
        return k % 2, 2 * h + (1 - flip if (k // 2) % 2 else flip), 1 - z1 if k // 4 else z1

    barrier = pltpu.get_barrier_semaphore()
    peers = [to_core, to_xh, to_yp, to_ym] + [to_xl] + [{"col": xl * 4 + rem(z + d, 4)} for d in range(1, 4)]
    for dev in peers:
        pl.semaphore_signal(barrier, inc=1, device_id=dev, device_id_type=MESH)

    @pl.when(jnp.logical_not(alone))
    def _():
        pl.semaphore_signal(barrier, inc=1, device_id=to_t, device_id_type=MESH)
        pl.semaphore_signal(barrier, inc=1, device_id=to_d, device_id_type=MESH)

    def local_vc():
        return pltpu.make_async_copy(refl, vc, vsem)

    local_vc().start()

    def s_copy(i, kk, m):
        return pltpu.make_async_copy(
            mat.at[2 * i + kk, 0, :, m, 0, :],
            sbuf.at[2 * i * (i + 1) + m, pl.ds(kk * 128, 128)],
            msem.at[2 * i + kk, m],
        )

    for i in range(4):
        @pl.loop(0, 4 * (i + 1))
        def _(m):
            s_copy(i, 0, m).start()
            s_copy(i, 1, m).start()

    local_vc().wait()
    for i in range(8):
        rows = pl.ds(i * 256, 256)
        vcs[0, rows, :], vcs[1, rows, :] = split(vc[rows, :])
    zero[...] = jnp.zeros_like(zero)

    def z_copy(i, kk, m):
        return pltpu.make_async_copy(zero, out.at[2 * i + kk, 0, :, m, 0, :], osem.at[2 * i + kk, m])

    def o_copy(i, kk, m):
        return pltpu.make_async_copy(
            sbuf.at[2 * i * (i + 1) + m, pl.ds(kk * 128, 128)],
            out.at[2 * i + kk, 0, :, m, 0, :],
            osem.at[2 * i + kk, m],
        )

    @pl.when(alone)
    def _():
        pl.semaphore_wait(barrier, len(peers))

    @pl.when(jnp.logical_not(alone))
    def _():
        pl.semaphore_wait(barrier, len(peers) + 2)

    def send(op, j, src, dst, dev):
        return pltpu.make_async_remote_copy(
            src_ref=src, dst_ref=dst, send_sem=ssem.at[j, OP[op]], recv_sem=rsem.at[j, OP[op]],
            device_id=dev, device_id_type=MESH,
        )

    sent = []

    def start(op, j, src, dst, dev):
        copy = send(op, j, src, dst, dev)
        copy.start()
        sent.append(copy)

    def got(op, j, dst):
        send(op, j, dst, dst, to_core).wait_recv()

    def v_copy(j):
        return send(
            "V0", j, refl.at[pl.ds(pl.multiple_of(own * 128, 128), 128), pl.ds(j * W, W)],
            vr.at[j, dz, dxl], to_d,
        )

    @pl.when(jnp.logical_not(alone))
    def _():
        for j in range(NC):
            v_copy(j).start()

    def diagonal(i):
        ia = lax.broadcasted_iota(jnp.int32, (256, 128), 0)
        ib = lax.broadcasted_iota(jnp.int32, (256, 128), 1)
        return (i * 2 + lax.shift_right_logical(ia, 7)) * 2048 + r * 128 + (ia & 127) - ib - c * 128

    def prep(i):
        line = diagonal(i)

        for m in range(4 * (i + 1)):
            s_copy(i, 0, m).wait()
            s_copy(i, 1, m).wait()
            x = sbuf[2 * i * (i + 1) + m]
            if m // 4 == i:
                gap = line - m * 1024
                x = jnp.where(gap > 0, x, jnp.where(gap == 0, 0.5 * x, 0.0))
            b = block(i, m // 4)
            cols = pl.ds((m % 4) * 128, 128)
            sh[b, :, cols], sl[b, :, cols] = split(x)

        @pl.loop(4 * (i + 1), 16)
        def _(m):
            z_copy(i, 0, m).start()
            z_copy(i, 1, m).start()

    def d_compute(i):
        acc = None
        for j in range(i + 1):
            b = block(i, j)
            rows = pl.ds(j * 512, 512)
            part = (
                dot(sh[b], vcs[0, rows, :]) + dot(sh[b], vcs[1, rows, :]) + dot(sl[b], vcs[0, rows, :])
            )
            acc = part if acc is None else acc + part
        rows = pl.ds(i * 256, 256)
        dh[rows, :], dl[rows, :] = split(acc)
        for kk in range(2):
            k = 2 * i + kk
            for j in range(NC):
                zk, xk = row_slot(k)
                dbuf[j, xk, zk] = acc[kk * 128:(kk + 1) * 128, j * W:(j + 1) * W]

    def v1(j):
        @pl.when(jnp.logical_not(alone))
        def _():
            got("V0", j, vr.at[j, z, xl])

        @pl.when(alone)
        def _():
            vr[j, z, xl] = vc[pl.ds(pl.multiple_of(own * 128, 128), 128), pl.ds(j * W, W)]

        start("V1", j, vr.at[j, z, xl], vr.at[j, z, xl], to_xl)

    def v2(j):
        got("V1", j, vr.at[j, z, 1 - xl])
        start("V2p", j, vr.at[j, z], vr.at[j, z], to_zp)
        start("V2m", j, vr.at[j, z], vr.at[j, z], to_zm)

    def v3(j):
        got("V2p", j, vr.at[j, zm])
        start("V3p", j, vr.at[j, zm, 0], vr.at[j, zm, 0], to_zp)
        got("V2m", j, vr.at[j, zp])
        start("V3m", j, vr.at[j, zp, 1], vr.at[j, zp, 1], to_zm)

    def v4(j):
        got("V3p", j, vr.at[j, z2, 0])
        got("V3m", j, vr.at[j, z2, 1])

    def t_compute(j):
        for k in range(8):
            zk, xk = row_slot(k)
            x = vr[j, zk, xk]
            i, kk = k // 2, k % 2
            rows, cols = pl.ds(kk * 128, 128), pl.ds(j * W, W)
            vrs[i, 0, rows, cols], vrs[i, 1, rows, cols] = split(x)
            xt = x.T
            cols = pl.ds(k * 128, 128)
            vrt[0:W, cols], vrt[W:2 * W, cols] = split(xt)
        for jj in range(4):
            acc = None
            for i in range(jj, 4):
                b = block(i, jj)
                cols = pl.ds(i * 256, 256)
                both = dot(vrt[:, cols], sh[b])
                part = both[:W] + both[W:] + dot(vrt[0:W, cols], sl[b])
                acc = part if acc is None else acc + part
            for mi in range(4):
                k0, yy, k1 = col_slot(4 * jj + mi)
                ubuf[j, k0, yy, k1, 0:W, :] = acc[:, mi * 128:(mi + 1) * 128]
        both = dot(vrt[...], dh[...])
        acc = both[:W] + both[W:] + dot(vrt[0:W, :], dl[...])
        for m in range(16):
            q = m % 4
            ubuf[j, m // 8, (m // 2) % 4, m % 2, W:UW, :] = (
                acc[q * Q:(q + 1) * Q, (m // 4) * 128:(m // 4 + 1) * 128]
            )

    first, second = pl.ds(0, 64), pl.ds(64, 64)

    def d1(j):
        start("D1", j, dbuf.at[j, 1 - xl], d2r.at[j], to_xl)

    def dx(j):
        got("D1", j, d2r.at[j])
        dbuf[j, xl, z2] = dbuf[j, xl, z2] + d2r[j, z2]
        start("D2p", j, dbuf.at[j, xl, z2, first], dr.at[j, 0], to_zp)
        start("D2m", j, dbuf.at[j, xl, z2, second], dr.at[j, 2], to_zm)
        dbuf[j, xl, zp] = dbuf[j, xl, zp] + d2r[j, zp]
        dbuf[j, xl, zm] = dbuf[j, xl, zm] + d2r[j, zm]
        start("D3p", j, dbuf.at[j, xl, zp, second], dr.at[j, 1], to_zp)
        start("D3m", j, dbuf.at[j, xl, zm, first], dr.at[j, 3], to_zm)
        dbuf[j, xl, z] = dbuf[j, xl, z] + d2r[j, z]

    def d2(j):
        got("D2p", j, dr.at[j, 0])
        dbuf[j, xl, zp, first] = dbuf[j, xl, zp, first] + dr[j, 0]
        start("D5p", j, dbuf.at[j, xl, zp, first], dr.at[j, 4], to_zp)
        got("D2m", j, dr.at[j, 2])
        dbuf[j, xl, zm, second] = dbuf[j, xl, zm, second] + dr[j, 2]
        start("D5m", j, dbuf.at[j, xl, zm, second], dr.at[j, 5], to_zm)

    def d3(j):
        got("D3p", j, dr.at[j, 1])
        got("D3m", j, dr.at[j, 3])
        got("D5p", j, dr.at[j, 4])
        dbuf[j, xl, z, first] = dbuf[j, xl, z, first] + dr[j, 3] + dr[j, 4]
        got("D5m", j, dr.at[j, 5])
        dbuf[j, xl, z, second] = dbuf[j, xl, z, second] + dr[j, 1] + dr[j, 5]

        @pl.when(jnp.logical_not(alone))
        def _():
            send("CD", j, dbuf.at[j, xl, z], crd.at[j], to_t).start()

    def t1(j):
        start("T1", j, ubuf.at[j, 1 - core], t1r.at[j], to_core)

    def t2(j):
        got("T1", j, t1r.at[j])
        ubuf[j, core, y2] = ubuf[j, core, y2] + t1r[j, y2]
        start("T2p", j, ubuf.at[j, core, y2, 0], t2r.at[j, 0], to_yp)
        start("T2m", j, ubuf.at[j, core, y2, 1], t2r.at[j, 2], to_ym)
        ubuf[j, core, yp] = ubuf[j, core, yp] + t1r[j, yp]
        ubuf[j, core, ym] = ubuf[j, core, ym] + t1r[j, ym]
        start("T3p", j, ubuf.at[j, core, yp, 1], t2r.at[j, 1], to_yp)
        start("T3m", j, ubuf.at[j, core, ym, 0], t2r.at[j, 3], to_ym)
        ubuf[j, core, y] = ubuf[j, core, y] + t1r[j, y]

    def t3(j):
        got("T2p", j, t2r.at[j, 0])
        ubuf[j, core, yp, 0] = ubuf[j, core, yp, 0] + t2r[j, 0]
        start("T5p", j, ubuf.at[j, core, yp, 0], t2r.at[j, 4], to_yp)
        got("T2m", j, t2r.at[j, 2])
        ubuf[j, core, ym, 1] = ubuf[j, core, ym, 1] + t2r[j, 2]
        start("T5m", j, ubuf.at[j, core, ym, 1], t2r.at[j, 5], to_ym)

    def t4(j):
        got("T3p", j, t2r.at[j, 1])
        got("T3m", j, t2r.at[j, 3])
        got("T5p", j, t2r.at[j, 4])
        ubuf[j, core, y, 0] = ubuf[j, core, y, 0] + t2r[j, 3] + t2r[j, 4]
        got("T5m", j, t2r.at[j, 5])
        ubuf[j, core, y, 1] = ubuf[j, core, y, 1] + t2r[j, 1] + t2r[j, 5]
        start("T4", j, ubuf.at[j, core, y, 1 - xh], t3r.at[j], to_xh)

    def t5(j):
        got("T4", j, t3r.at[j])
        ubuf[j, core, y, xh] = ubuf[j, core, y, xh] + t3r[j]

        @pl.when(jnp.logical_not(alone))
        def _():
            send("CT", j, ubuf.at[j, core, y, xh, 0:W], crt.at[j], to_d).start()

        start("R1", j, ubuf.at[j, core, y, xh, W:UW], rx.at[j, 0], to_xl)

    def rz(j):
        got("R1", j, rx.at[j, 0])
        rx[j, 1] = ubuf[j, core, y, xh, W:UW, :] + rx[j, 0]
        for d in range(1, 4):
            start(f"R{d + 1}", j, rx.at[j, 1], rx.at[j, 1 + d], {"col": xl * 4 + rem(z + d, 4)})

    def join(j):
        @pl.when(jnp.logical_not(alone))
        def _():
            got("CD", j, crd.at[j])
            got("CT", j, crt.at[j])

        @pl.when(alone)
        def _():
            crd[j] = dbuf[j, xl, z]
            crt[j] = ubuf[j, core, y, xh, 0:W, :]

        wr[j, z, xl] = dbuf[j, xl, z] + crt[j].T
        start("B1", j, wr.at[j, z, xl], wr.at[j, z, xl], to_xl)
        gbuf[j, core, y, xh, 0:W, :] = ubuf[j, core, y, xh, 0:W, :] + crd[j].T
        total = rx[j, 1]
        for d in range(1, 4):
            got(f"R{d + 1}", j, rx.at[j, 1 + d])
            total = total + rx[j, 1 + d]
        gbuf[j, core, y, xh, W:UW, :] = total
        start("A1", j, gbuf.at[j, core, y, xh], gbuf.at[j, core, y, xh], to_xh)

    def a2(j):
        got("B1", j, wr.at[j, z, 1 - xl])
        start("B2p", j, wr.at[j, z], wr.at[j, z], to_zp)
        start("B2m", j, wr.at[j, z], wr.at[j, z], to_zm)
        got("A1", j, gbuf.at[j, core, y, 1 - xh])
        start("A2p", j, gbuf.at[j, core, y], gbuf.at[j, core, y], to_yp)
        start("A2m", j, gbuf.at[j, core, y], gbuf.at[j, core, y], to_ym)

    def a3(j):
        got("B2p", j, wr.at[j, zm])
        start("B3p", j, wr.at[j, zm, 0], wr.at[j, zm, 0], to_zp)
        got("B2m", j, wr.at[j, zp])
        start("B3m", j, wr.at[j, zp, 1], wr.at[j, zp, 1], to_zm)
        got("A2p", j, gbuf.at[j, core, ym])
        start("A3p", j, gbuf.at[j, core, ym, 0], gbuf.at[j, core, ym, 0], to_yp)
        got("A2m", j, gbuf.at[j, core, yp])
        start("A3m", j, gbuf.at[j, core, yp, 1], gbuf.at[j, core, yp, 1], to_ym)

    def a4(j):
        got("A3p", j, gbuf.at[j, core, y2, 0])
        got("A3m", j, gbuf.at[j, core, y2, 1])
        start("A4", j, gbuf.at[j, core], gbuf.at[j, core], to_core)
        got("B3p", j, wr.at[j, z2, 0])
        got("B3m", j, wr.at[j, z2, 1])

    def a5(j):
        got("A4", j, gbuf.at[j, 1 - core])
        for m in range(16):
            k0, yy, k1 = col_slot(m)
            rows, cols = pl.ds(j * W, W), pl.ds(m * 128, 128)
            wcts[0, rows, cols], wcts[1, rows, cols] = split(gbuf[j, k0, yy, k1, 0:W, :])
            q = m % 4
            mm[pl.ds(j * W + q * Q, Q), pl.ds((m // 4) * 128, 128)] = (
                gbuf[j, m // 8, (m // 2) % 4, m % 2, W:UW, :]
            )

    def v_ready(j):
        v4(j)
        t_compute(j)
        t1(j)

    stages = {
        "prep": prep, "dc": d_compute, "v1": v1, "v2": v2, "v3": v3, "vt": v_ready,
        "d1": d1, "dx": dx, "d2": d2, "d3": d3, "t2": t2, "t3": t3, "t4": t4, "t5": t5, "rz": rz,
        "cx": join, "a2": a2, "a3": a3, "a4": a4, "a5": a5,
    }
    for name, order in PLAN:
        for n in order:
            stages[name](n)

    m_sum = mm[...] + mm[...].T
    mh, ml = split(m_sum)
    for i in range(4):
        both = dot(vrs[i].reshape(RANK, RANK), mh)
        fix = both[:256] + both[256:] + dot(vrs[i, 0], ml)
        for kk in range(2):
            k = 2 * i + kk
            for j in range(NC):
                zk, xk = row_slot(k)
                x = wr[j, zk, xk] - fix[kk * 128:(kk + 1) * 128, j * W:(j + 1) * W]
                rows, cols = pl.ds(kk * 128, 128), pl.ds(j * W, W)
                wrs[i, 0, rows, cols], wrs[i, 1, rows, cols] = split(x)
        for j in range(i + 1):
            part = pl.ds(j * 512, 512)
            both = dot(vrs[i].reshape(512, RANK), wcts[0, :, part])
            both = both + dot_nt(wrs[i].reshape(512, RANK), vcs[0, part, :])
            delta = (
                both[:256] + both[256:] + dot(vrs[i, 0], wcts[1, :, part]) + dot_nt(wrs[i, 0], vcs[1, part, :])
            )
            for mi in range(4):
                m = 4 * j + mi
                x = sbuf[2 * i * (i + 1) + m] - delta[:, mi * 128:(mi + 1) * 128]
                if i == j:
                    x = jnp.where(diagonal(i) >= m * 1024, x, 0.0)
                sbuf[2 * i * (i + 1) + m] = x
                for kk in range(2):
                    o_copy(i, kk, m).start()
    for copy in sent:
        copy.wait_send()

    @pl.when(jnp.logical_not(alone))
    def _():
        for j in range(NC):
            v_copy(j).wait_send()
            send("CD", j, dbuf.at[j, xl, z], crd.at[j], to_t).wait_send()
            send("CT", j, ubuf.at[j, core, y, xh, 0:W], crt.at[j], to_d).wait_send()

    for i in range(4):
        @pl.loop(0, 4 * (i + 1))
        def _(m):
            o_copy(i, 0, m).wait()
            o_copy(i, 1, m).wait()

        @pl.loop(4 * (i + 1), 16)
        def _(m):
            z_copy(i, 0, m).wait()
            z_copy(i, 1, m).wait()


def project(mat, refl):
    vm = pltpu.VMEM
    scratch = [
        vm((40, 256, 128), F32),
        vm((10, 256, 512), BF16),
        vm((10, 256, 512), BF16),
        vm((2048, RANK), F32),
        vm((2, 2048, RANK), BF16),
        vm((NC, 4, 2, 128, W), F32),
        vm((4, 2, 256, RANK), BF16),
        vm((2 * W, 1024), BF16),
        vm((NC, 2, 4, 128, W), F32),
        vm((1024, RANK), BF16),
        vm((1024, RANK), BF16),
        vm((NC, 6, 64, W), F32),
        vm((NC, 4, 128, W), F32),
        vm((NC, 2, 4, 2, UW, 128), F32),
        vm((NC, 4, 2, UW, 128), F32),
        vm((NC, 6, UW, 128), F32),
        vm((NC, UW, 128), F32),
        vm((NC, 128, W), F32),
        vm((NC, W, 128), F32),
        vm((NC, 5, Q, 128), F32),
        vm((NC, 2, 4, 2, UW, 128), F32),
        vm((NC, 4, 2, 128, W), F32),
        vm((RANK, RANK), F32),
        vm((2, RANK, 2048), BF16),
        vm((4, 2, 256, RANK), BF16),
        vm((128, 128), F32),
        pltpu.SemaphoreType.DMA((NC, len(OPS))),
        pltpu.SemaphoreType.DMA((NC, len(OPS))),
        pltpu.SemaphoreType.DMA((8, 16)),
        pltpu.SemaphoreType.DMA,
        pltpu.SemaphoreType.DMA((8, 16)),
    ]
    hbm = pl.BlockSpec(memory_space=pltpu.HBM)
    return pl.pallas_call(
        exchange,
        out_shape=jax.ShapeDtypeStruct(mat.shape, F32),
        in_specs=[hbm, hbm],
        out_specs=hbm,
        scratch_shapes=scratch,
        compiler_params=pltpu.CompilerParams(
            collective_id=0, has_side_effects=True, vmem_limit_bytes=67043328
        ),
        name="exchange",
    )(mat, refl)


def per_device(matrix, reflectors):
    refl = reflectors.reshape(2048, RANK)
    return project(matrix, refl)


def solution(mesh):
    placed = (P(None, "row", None, None, "col", None), P(None, "col", None, None))
    return jax.shard_map(
        per_device,
        mesh=mesh,
        in_specs=placed,
        out_specs=P(None, "row", None, None, "col", None),
        check_vma=False,
    )
```

```python
import jax
import jax.numpy as jnp
from jax import lax
from jax.experimental import pallas as pl
from jax.experimental.pallas import tpu as pltpu
from jax.sharding import PartitionSpec as P

MESH = pl.DeviceIdType.MESH
F32 = jnp.float32
BF16 = jnp.bfloat16
NC = 4
PLAN = (
    ("prep", (3, 2, 1)), ("dc", (2,)), ("v1", (0,)), ("dc", (1,)), ("v1", (1,)), ("prep", (0,)), ("dc", (0,)),
    ("v1", (2,)), ("v2", (0,)), ("v1", (3,)), ("dc", (3,)), ("v2", (2,)), ("d1", (0, 2)), ("v3", (0, 2)),
    ("v2", (3, 1)), ("vt", (0, 2)), ("d1", (3, 1)), ("t2", (0,)), ("v3", (3,)), ("dx", (0,)), ("t2", (2,)),
    ("t3", (0,)), ("vt", (3,)), ("v3", (1,)), ("t3", (2,)), ("d2", (0,)), ("dx", (2, 3)), ("t2", (3,)), ("t4", (0,)),
    ("d2", (2,)), ("t4", (2,)), ("d3", (0,)), ("vt", (1,)), ("t3", (3,)), ("t5", (0,)), ("d2", (3,)), ("t5", (2,)),
    ("d3", (2,)), ("t2", (1,)), ("rz", (0,)), ("dx", (1,)), ("t4", (3,)), ("d3", (3,)), ("cb", (0,)), ("rz", (2,)),
    ("t3", (1,)), ("d2", (1,)), ("ca", (0,)), ("t5", (3,)), ("cb", (2,)), ("t4", (1,)), ("ca", (2,)), ("rz", (3,)),
    ("d3", (1,)), ("a2", (0,)), ("t5", (1,)), ("cb", (3,)), ("ca", (3,)), ("a2", (2,)), ("rz", (1,)), ("a3", (0,)),
    ("b2", (0,)), ("cb", (1,)), ("ca", (1,)), ("b2", (2,)), ("a2", (3,)), ("a3", (2,)), ("b2", (3,)), ("a2", (1,)),
    ("a4", (0,)), ("b3", (0, 2)), ("b2", (1,)), ("a4", (2,)), ("a5", (0,)), ("b3", (3,)), ("a3", (3, 1)),
    ("a4", (3,)), ("b4", (0,)), ("b3", (1,)), ("a4", (1,)), ("a5", (3, 2)), ("b4", (1,)), ("a5", (1,)),
    ("b4", (2, 3)),
)
RANK = 512
W = RANK // NC
Q = W // 4
UW = W + Q

RINGS = ("V", "A", "B", "D", "T")
OPS = [a + b for a in RINGS for b in ("1", "2p", "2m", "3p", "3m", "4", "5p", "5m")]
OPS += ["V0", "CD", "CT"] + ["R1", "R2", "R3", "R4"]
OP = {name: n for n, name in enumerate(OPS)}


def split(x):
    hi = x.astype(BF16)
    return hi, (x - hi.astype(F32)).astype(BF16)


def dot(a, b):
    return jnp.dot(a, b, preferred_element_type=F32)


def dot_nt(a, b):
    return lax.dot_general(a, b, (((1,), (1,)), ((), ())), preferred_element_type=F32)


def block(i, j):
    return i * (i + 1) // 2 + j


def xor(a, b):
    return a + b - 2 * a * b


def exchange(
    mat, refl, out,
    sbuf, sh, sl, vc, vcs, vr, vrs, vrt, dbuf, dh, dl, dr, d2r,
    ubuf, t1r, t2r, t3r, crd, crt, rx, gbuf, wr, mm, wcts, wrs,
    ssem, rsem, msem, vsem, osem,
):
    r, c = lax.axis_index("row"), lax.axis_index("col")
    div, rem = lax.div, lax.rem
    core, y = rem(r, 2), div(r, 4)
    xh = rem(div(r, 2), 2)
    z, xl = rem(c, 4), div(c, 4)
    half, low = div(r, 8), rem(r, 8)
    alone = low == c
    y0, z1, z0 = rem(y, 2), div(z, 2), rem(z, 2)
    yp, ym, y2 = rem(y + 1, 4), rem(y + 3, 4), rem(y + 2, 4)
    zp, zm, z2 = rem(z + 1, 4), rem(z + 3, 4), rem(z + 2, 4)
    to_core = {"row": r + 1 - 2 * core}
    to_xh = {"row": r + 2 - 4 * xh}
    to_yp, to_ym = {"row": yp * 4 + rem(r, 4)}, {"row": ym * 4 + rem(r, 4)}
    to_xl = {"col": c + 4 - 8 * xl}
    to_zp, to_zm = {"col": xl * 4 + zp}, {"col": xl * 4 + zm}
    flip = xor(z1, xl)
    to_t = {"row": half * 8 + 4 * xor(xor(z1, xh), y0) + 2 * xor(xor(xl, y0), xh) + z0, "col": low}
    dxl, dz1 = xor(xh, flip), xor(y0, flip)
    to_d = {"row": half * 8 + c, "col": dxl * 4 + dz1 * 2 + core}
    dz = dz1 * 2 + core
    own = 2 * (4 * xor(xh, z1) + 2 * dz1 + core) + half

    def row_slot(k):
        return k % 4, 1 - y0 if k // 4 else y0

    def col_slot(m):
        k, h = m // 2, m % 2
        return k % 2, 2 * h + (1 - flip if (k // 2) % 2 else flip), 1 - z1 if k // 4 else z1

    barrier = pltpu.get_barrier_semaphore()
    peers = [to_core, to_xh, to_yp, to_ym] + [to_xl] + [{"col": xl * 4 + rem(z + d, 4)} for d in range(1, 4)]
    for dev in peers:
        pl.semaphore_signal(barrier, inc=1, device_id=dev, device_id_type=MESH)

    @pl.when(jnp.logical_not(alone))
    def _():
        pl.semaphore_signal(barrier, inc=1, device_id=to_t, device_id_type=MESH)
        pl.semaphore_signal(barrier, inc=1, device_id=to_d, device_id_type=MESH)

    def local_vc():
        return pltpu.make_async_copy(refl, vc, vsem)

    local_vc().start()

    def s_copy(i, kk, m):
        return pltpu.make_async_copy(
            mat.at[2 * i + kk, 0, :, m, 0, :],
            sbuf.at[2 * i * (i + 1) + m, pl.ds(kk * 128, 128)],
            msem.at[2 * i + kk, m],
        )

    for i in range(4):
        @pl.loop(0, 4 * (i + 1))
        def _(m):
            s_copy(i, 0, m).start()
            s_copy(i, 1, m).start()

    local_vc().wait()
    for i in range(8):
        rows = pl.ds(i * 256, 256)
        vcs[0, rows, :], vcs[1, rows, :] = split(vc[rows, :])
    def o_copy(i, m):
        spot = 2 * i * (i + 1) + m
        return pltpu.make_async_copy(sbuf.at[spot], out.at[spot], osem.at[i, m])

    @pl.when(alone)
    def _():
        pl.semaphore_wait(barrier, len(peers))

    @pl.when(jnp.logical_not(alone))
    def _():
        pl.semaphore_wait(barrier, len(peers) + 2)

    def send(op, j, src, dst, dev):
        return pltpu.make_async_remote_copy(
            src_ref=src, dst_ref=dst, send_sem=ssem.at[j, OP[op]], recv_sem=rsem.at[j, OP[op]],
            device_id=dev, device_id_type=MESH,
        )

    sent = []

    def start(op, j, src, dst, dev):
        copy = send(op, j, src, dst, dev)
        copy.start()
        sent.append(copy)

    def got(op, j, dst):
        send(op, j, dst, dst, to_core).wait_recv()

    def v_copy(j):
        return send(
            "V0", j, vc.at[pl.ds(pl.multiple_of(own * 128, 128), 128), pl.ds(j * W, W)],
            vr.at[j, dz, dxl], to_d,
        )

    @pl.when(jnp.logical_not(alone))
    def _():
        for j in range(NC):
            v_copy(j).start()

    def diagonal(i):
        ia = lax.broadcasted_iota(jnp.int32, (256, 128), 0)
        ib = lax.broadcasted_iota(jnp.int32, (256, 128), 1)
        return (i * 2 + lax.shift_right_logical(ia, 7)) * 2048 + r * 128 + (ia & 127) - ib - c * 128

    def prep(i):
        line = diagonal(i)

        for m in range(4 * (i + 1)):
            s_copy(i, 0, m).wait()
            s_copy(i, 1, m).wait()
            x = sbuf[2 * i * (i + 1) + m]
            if m // 4 == i:
                gap = line - m * 1024
                x = jnp.where(gap > 0, x, jnp.where(gap == 0, 0.5 * x, 0.0))
            b = block(i, m // 4)
            cols = pl.ds((m % 4) * 128, 128)
            sh[b, :, cols], sl[b, :, cols] = split(x)

    def d_compute(i):
        acc = None
        for j in range(i + 1):
            b = block(i, j)
            rows = pl.ds(j * 512, 512)
            part = (
                dot(sh[b], vcs[0, rows, :]) + dot(sh[b], vcs[1, rows, :]) + dot(sl[b], vcs[0, rows, :])
            )
            acc = part if acc is None else acc + part
        rows = pl.ds(i * 256, 256)
        dh[rows, :], dl[rows, :] = split(acc)
        for kk in range(2):
            k = 2 * i + kk
            for j in range(NC):
                zk, xk = row_slot(k)
                dbuf[j, xk, zk] = acc[kk * 128:(kk + 1) * 128, j * W:(j + 1) * W]

    def v1(j):
        @pl.when(jnp.logical_not(alone))
        def _():
            got("V0", j, vr.at[j, z, xl])

        @pl.when(alone)
        def _():
            vr[j, z, xl] = vc[pl.ds(pl.multiple_of(own * 128, 128), 128), pl.ds(j * W, W)]

        start("V1", j, vr.at[j, z, xl], vr.at[j, z, xl], to_xl)

    def v2(j):
        got("V1", j, vr.at[j, z, 1 - xl])
        start("V2p", j, vr.at[j, z], vr.at[j, z], to_zp)
        start("V2m", j, vr.at[j, z], vr.at[j, z], to_zm)

    def v3(j):
        got("V2p", j, vr.at[j, zm])
        start("V3p", j, vr.at[j, zm, 0], vr.at[j, zm, 0], to_zp)
        got("V2m", j, vr.at[j, zp])
        start("V3m", j, vr.at[j, zp, 1], vr.at[j, zp, 1], to_zm)

    def v4(j):
        got("V3p", j, vr.at[j, z2, 0])
        got("V3m", j, vr.at[j, z2, 1])

    def t_compute(j):
        for k in range(8):
            zk, xk = row_slot(k)
            x = vr[j, zk, xk]
            i, kk = k // 2, k % 2
            rows, cols = pl.ds(kk * 128, 128), pl.ds(j * W, W)
            vrs[i, 0, rows, cols], vrs[i, 1, rows, cols] = split(x)
            xt = x.T
            cols = pl.ds(k * 128, 128)
            vrt[0:W, cols], vrt[W:2 * W, cols] = split(xt)
        for jj in range(4):
            acc = None
            for i in range(jj, 4):
                b = block(i, jj)
                cols = pl.ds(i * 256, 256)
                both = dot(vrt[:, cols], sh[b])
                part = both[:W] + both[W:] + dot(vrt[0:W, cols], sl[b])
                acc = part if acc is None else acc + part
            for mi in range(4):
                k0, yy, k1 = col_slot(4 * jj + mi)
                ubuf[j, k0, yy, k1, 0:W, :] = acc[:, mi * 128:(mi + 1) * 128]
        both = dot(vrt[...], dh[...])
        acc = both[:W] + both[W:] + dot(vrt[0:W, :], dl[...])
        for m in range(16):
            q = m % 4
            ubuf[j, m // 8, (m // 2) % 4, m % 2, W:UW, :] = (
                acc[q * Q:(q + 1) * Q, (m // 4) * 128:(m // 4 + 1) * 128]
            )

    first, second = pl.ds(0, 64), pl.ds(64, 64)

    def d1(j):
        start("D1", j, dbuf.at[j, 1 - xl], d2r.at[j], to_xl)

    def dx(j):
        got("D1", j, d2r.at[j])
        dbuf[j, xl, z2] = dbuf[j, xl, z2] + d2r[j, z2]
        start("D2p", j, dbuf.at[j, xl, z2, first], dr.at[j, 0], to_zp)
        start("D2m", j, dbuf.at[j, xl, z2, second], dr.at[j, 2], to_zm)
        dbuf[j, xl, zp] = dbuf[j, xl, zp] + d2r[j, zp]
        dbuf[j, xl, zm] = dbuf[j, xl, zm] + d2r[j, zm]
        start("D3p", j, dbuf.at[j, xl, zp, second], dr.at[j, 1], to_zp)
        start("D3m", j, dbuf.at[j, xl, zm, first], dr.at[j, 3], to_zm)
        dbuf[j, xl, z] = dbuf[j, xl, z] + d2r[j, z]

    def d2(j):
        got("D2p", j, dr.at[j, 0])
        dbuf[j, xl, zp, first] = dbuf[j, xl, zp, first] + dr[j, 0]
        start("D5p", j, dbuf.at[j, xl, zp, first], dr.at[j, 4], to_zp)
        got("D2m", j, dr.at[j, 2])
        dbuf[j, xl, zm, second] = dbuf[j, xl, zm, second] + dr[j, 2]
        start("D5m", j, dbuf.at[j, xl, zm, second], dr.at[j, 5], to_zm)

    def d3(j):
        got("D3p", j, dr.at[j, 1])
        got("D3m", j, dr.at[j, 3])
        got("D5p", j, dr.at[j, 4])
        dbuf[j, xl, z, first] = dbuf[j, xl, z, first] + dr[j, 3] + dr[j, 4]
        got("D5m", j, dr.at[j, 5])
        dbuf[j, xl, z, second] = dbuf[j, xl, z, second] + dr[j, 1] + dr[j, 5]

        @pl.when(jnp.logical_not(alone))
        def _():
            send("CD", j, dbuf.at[j, xl, z], crd.at[j], to_t).start()

    def t1(j):
        start("T1", j, ubuf.at[j, 1 - core], t1r.at[j], to_core)

    def t2(j):
        got("T1", j, t1r.at[j])
        ubuf[j, core, y2] = ubuf[j, core, y2] + t1r[j, y2]
        start("T2p", j, ubuf.at[j, core, y2, 0], t2r.at[j, 0], to_yp)
        start("T2m", j, ubuf.at[j, core, y2, 1], t2r.at[j, 2], to_ym)
        ubuf[j, core, yp] = ubuf[j, core, yp] + t1r[j, yp]
        ubuf[j, core, ym] = ubuf[j, core, ym] + t1r[j, ym]
        start("T3p", j, ubuf.at[j, core, yp, 1], t2r.at[j, 1], to_yp)
        start("T3m", j, ubuf.at[j, core, ym, 0], t2r.at[j, 3], to_ym)
        ubuf[j, core, y] = ubuf[j, core, y] + t1r[j, y]

    def t3(j):
        got("T2p", j, t2r.at[j, 0])
        ubuf[j, core, yp, 0] = ubuf[j, core, yp, 0] + t2r[j, 0]
        start("T5p", j, ubuf.at[j, core, yp, 0], t2r.at[j, 4], to_yp)
        got("T2m", j, t2r.at[j, 2])
        ubuf[j, core, ym, 1] = ubuf[j, core, ym, 1] + t2r[j, 2]
        start("T5m", j, ubuf.at[j, core, ym, 1], t2r.at[j, 5], to_ym)

    def t4(j):
        got("T3p", j, t2r.at[j, 1])
        got("T3m", j, t2r.at[j, 3])
        got("T5p", j, t2r.at[j, 4])
        ubuf[j, core, y, 0] = ubuf[j, core, y, 0] + t2r[j, 3] + t2r[j, 4]
        got("T5m", j, t2r.at[j, 5])
        ubuf[j, core, y, 1] = ubuf[j, core, y, 1] + t2r[j, 1] + t2r[j, 5]
        start("T4", j, ubuf.at[j, core, y, 1 - xh], t3r.at[j], to_xh)

    def t5(j):
        got("T4", j, t3r.at[j])
        ubuf[j, core, y, xh] = ubuf[j, core, y, xh] + t3r[j]

        @pl.when(jnp.logical_not(alone))
        def _():
            send("CT", j, ubuf.at[j, core, y, xh, 0:W], crt.at[j], to_d).start()

        start("R1", j, ubuf.at[j, core, y, xh, W:UW], rx.at[j, 0], to_xl)

    def rz(j):
        got("R1", j, rx.at[j, 0])
        rx[j, 1] = ubuf[j, core, y, xh, W:UW, :] + rx[j, 0]
        for d in range(1, 4):
            start(f"R{d + 1}", j, rx.at[j, 1], rx.at[j, 1 + d], {"col": xl * 4 + rem(z + d, 4)})

    def join_b(j):
        @pl.when(jnp.logical_not(alone))
        def _():
            got("CD", j, crd.at[j])
            got("CT", j, crt.at[j])

        @pl.when(alone)
        def _():
            crd[j] = dbuf[j, xl, z]
            crt[j] = ubuf[j, core, y, xh, 0:W, :]

        wr[j, z, xl] = dbuf[j, xl, z] + crt[j].T
        start("B1", j, wr.at[j, z, xl], wr.at[j, z, xl], to_xl)
        gbuf[j, core, y, xh, 0:W, :] = ubuf[j, core, y, xh, 0:W, :] + crd[j].T

    def join_a(j):
        total = rx[j, 1]
        for d in range(1, 4):
            got(f"R{d + 1}", j, rx.at[j, 1 + d])
            total = total + rx[j, 1 + d]
        gbuf[j, core, y, xh, W:UW, :] = total
        start("A1", j, gbuf.at[j, core, y, xh], gbuf.at[j, core, y, xh], to_xh)

    def b2(j):
        got("B1", j, wr.at[j, z, 1 - xl])
        start("B2p", j, wr.at[j, z], wr.at[j, z], to_zp)
        start("B2m", j, wr.at[j, z], wr.at[j, z], to_zm)

    def a2(j):
        got("A1", j, gbuf.at[j, core, y, 1 - xh])
        start("A2p", j, gbuf.at[j, core, y], gbuf.at[j, core, y], to_yp)
        start("A2m", j, gbuf.at[j, core, y], gbuf.at[j, core, y], to_ym)

    def b3(j):
        got("B2p", j, wr.at[j, zm])
        start("B3p", j, wr.at[j, zm, 0], wr.at[j, zm, 0], to_zp)
        got("B2m", j, wr.at[j, zp])
        start("B3m", j, wr.at[j, zp, 1], wr.at[j, zp, 1], to_zm)

    def a3(j):
        got("A2p", j, gbuf.at[j, core, ym])
        start("A3p", j, gbuf.at[j, core, ym, 0], gbuf.at[j, core, ym, 0], to_yp)
        got("A2m", j, gbuf.at[j, core, yp])
        start("A3m", j, gbuf.at[j, core, yp, 1], gbuf.at[j, core, yp, 1], to_ym)

    def a4(j):
        got("A3p", j, gbuf.at[j, core, y2, 0])
        got("A3m", j, gbuf.at[j, core, y2, 1])
        start("A4", j, gbuf.at[j, core], gbuf.at[j, core], to_core)

    def b4(j):
        got("B3p", j, wr.at[j, z2, 0])
        got("B3m", j, wr.at[j, z2, 1])

    def a5(j):
        got("A4", j, gbuf.at[j, 1 - core])
        for m in range(16):
            k0, yy, k1 = col_slot(m)
            rows, cols = pl.ds(j * W, W), pl.ds(m * 128, 128)
            wcts[0, rows, cols], wcts[1, rows, cols] = split(gbuf[j, k0, yy, k1, 0:W, :])
            q = m % 4
            mm[pl.ds(j * W + q * Q, Q), pl.ds((m // 4) * 128, 128)] = (
                gbuf[j, m // 8, (m // 2) % 4, m % 2, W:UW, :]
            )

    def v_ready(j):
        v4(j)
        t_compute(j)
        t1(j)

    stages = {
        "prep": prep, "dc": d_compute, "v1": v1, "v2": v2, "v3": v3, "vt": v_ready,
        "d1": d1, "dx": dx, "d2": d2, "d3": d3, "t2": t2, "t3": t3, "t4": t4, "t5": t5, "rz": rz,
        "cb": join_b, "ca": join_a, "b2": b2, "b3": b3, "b4": b4, "a2": a2, "a3": a3, "a4": a4, "a5": a5,
    }
    for name, order in PLAN:
        for n in order:
            stages[name](n)

    m_sum = mm[...] + mm[...].T
    mh, ml = split(m_sum)
    for i in range(4):
        both = dot(vrs[i].reshape(RANK, RANK), mh)
        fix = both[:256] + both[256:] + dot(vrs[i, 0], ml)
        for kk in range(2):
            k = 2 * i + kk
            for j in range(NC):
                zk, xk = row_slot(k)
                x = wr[j, zk, xk] - fix[kk * 128:(kk + 1) * 128, j * W:(j + 1) * W]
                rows, cols = pl.ds(kk * 128, 128), pl.ds(j * W, W)
                wrs[i, 0, rows, cols], wrs[i, 1, rows, cols] = split(x)
        for j in range(i + 1):
            part = pl.ds(j * 512, 512)
            both = dot(vrs[i].reshape(512, RANK), wcts[0, :, part])
            both = both + dot_nt(wrs[i].reshape(512, RANK), vcs[0, part, :])
            delta = (
                both[:256] + both[256:] + dot(vrs[i, 0], wcts[1, :, part]) + dot_nt(wrs[i, 0], vcs[1, part, :])
            )
            for mi in range(4):
                m = 4 * j + mi
                x = sbuf[2 * i * (i + 1) + m] - delta[:, mi * 128:(mi + 1) * 128]
                if i == j:
                    x = jnp.where(diagonal(i) >= m * 1024, x, 0.0)
                sbuf[2 * i * (i + 1) + m] = x
                o_copy(i, m).start()
    for copy in sent:
        copy.wait_send()

    @pl.when(jnp.logical_not(alone))
    def _():
        for j in range(NC):
            v_copy(j).wait_send()
            send("CD", j, dbuf.at[j, xl, z], crd.at[j], to_t).wait_send()
            send("CT", j, ubuf.at[j, core, y, xh, 0:W], crt.at[j], to_d).wait_send()

    for i in range(4):
        @pl.loop(0, 4 * (i + 1))
        def _(m):
            o_copy(i, m).wait()


def place(tiles, out, buf, zero, isem, osem):
    def fetch(n):
        return pltpu.make_async_copy(tiles.at[n], buf.at[n], isem.at[n])

    def put(i, kk, m):
        upper = m >= 4 * (i + 1)
        src = zero if upper else buf.at[2 * i * (i + 1) + m, pl.ds(kk * 128, 128)]
        return pltpu.make_async_copy(src, out.at[2 * i + kk, 0, :, m, 0, :], osem.at[2 * i + kk, m])

    for n in range(40):
        fetch(n).start()
    zero[...] = jnp.zeros_like(zero)
    every = [(i, m) for i in range(4) for m in range(16)]
    for i, m in every:
        if m >= 4 * (i + 1):
            put(i, 0, m).start()
            put(i, 1, m).start()
    for i, m in every:
        if m < 4 * (i + 1):
            fetch(2 * i * (i + 1) + m).wait()
            put(i, 0, m).start()
            put(i, 1, m).start()
    for i, m in every:
        put(i, 0, m).wait()
        put(i, 1, m).wait()


def spread(tiles, shape):
    hbm = pl.BlockSpec(memory_space=pltpu.HBM)
    return pl.pallas_call(
        place,
        out_shape=jax.ShapeDtypeStruct(shape, F32),
        in_specs=[hbm],
        out_specs=hbm,
        scratch_shapes=[
            pltpu.VMEM((40, 256, 128), F32),
            pltpu.VMEM((128, 128), F32),
            pltpu.SemaphoreType.DMA((40,)),
            pltpu.SemaphoreType.DMA((8, 16)),
        ],
        compiler_params=pltpu.CompilerParams(vmem_limit_bytes=67043328),
        name="place",
    )(tiles)


def project(mat, refl):
    vm = pltpu.VMEM
    scratch = [
        vm((40, 256, 128), F32),
        vm((10, 256, 512), BF16),
        vm((10, 256, 512), BF16),
        vm((2048, RANK), F32),
        vm((2, 2048, RANK), BF16),
        vm((NC, 4, 2, 128, W), F32),
        vm((4, 2, 256, RANK), BF16),
        vm((2 * W, 1024), BF16),
        vm((NC, 2, 4, 128, W), F32),
        vm((1024, RANK), BF16),
        vm((1024, RANK), BF16),
        vm((NC, 6, 64, W), F32),
        vm((NC, 4, 128, W), F32),
        vm((NC, 2, 4, 2, UW, 128), F32),
        vm((NC, 4, 2, UW, 128), F32),
        vm((NC, 6, UW, 128), F32),
        vm((NC, UW, 128), F32),
        vm((NC, 128, W), F32),
        vm((NC, W, 128), F32),
        vm((NC, 5, Q, 128), F32),
        vm((NC, 2, 4, 2, UW, 128), F32),
        vm((NC, 4, 2, 128, W), F32),
        vm((RANK, RANK), F32),
        vm((2, RANK, 2048), BF16),
        vm((4, 2, 256, RANK), BF16),
        pltpu.SemaphoreType.DMA((NC, len(OPS))),
        pltpu.SemaphoreType.DMA((NC, len(OPS))),
        pltpu.SemaphoreType.DMA((8, 16)),
        pltpu.SemaphoreType.DMA,
        pltpu.SemaphoreType.DMA((4, 16)),
    ]
    hbm = pl.BlockSpec(memory_space=pltpu.HBM)
    return pl.pallas_call(
        exchange,
        out_shape=jax.ShapeDtypeStruct((40, 256, 128), F32),
        in_specs=[hbm, hbm],
        out_specs=hbm,
        scratch_shapes=scratch,
        compiler_params=pltpu.CompilerParams(
            collective_id=0, has_side_effects=True, vmem_limit_bytes=67043328
        ),
        name="exchange",
    )(mat, refl)


def per_device(matrix, reflectors):
    refl = reflectors.reshape(2048, RANK)
    return spread(project(matrix, refl), matrix.shape)


def solution(mesh):
    placed = (P(None, "row", None, None, "col", None), P(None, "col", None, None))
    return jax.shard_map(
        per_device,
        mesh=mesh,
        in_specs=placed,
        out_specs=P(None, "row", None, None, "col", None),
        check_vma=False,
    )
```
